32 devices in a mesh: wide: 16 (over z, y, x), narrow: 2 (over core).
Axes of the slice: x: 2, y: 2, z: 4, core: 2. Of those that a mesh axis runs over, the one named last changes fastest.
Arguments:
- square_grads: bfloat16 [4, 8192, 8192], P(None, 'wide', 'narrow'), may hold values from -8.1 to 8.1
- narrow_grads: bfloat16 [4, 8192, 1024], P(None, 'wide', 'narrow'), may hold values from -8.1 to 8.1
- square_rowstate: float32 [4, 8192], P(None, 'wide'), may hold values from 0.0006 to 0.064
- square_colstate: float32 [4, 8192], P(None, 'narrow'), may hold values from 1e-05 to 2.1
- narrow_rowstate: float32 [4, 8192], P(None, 'wide'), may hold values from 0.0006 to 0.064
- narrow_colstate: float32 [4, 1024], P(None, 'narrow'), may hold values from 1e-05 to 2.1
Outputs:
- square_update: float32 [4, 8192, 8192], P(None, 'wide', 'narrow')
- narrow_update: float32 [4, 8192, 1024], P(None, 'wide', 'narrow')
- square_rowfactor: float32 [4, 8192], P(None, 'wide')
- square_colfactor: float32 [4, 8192], P(None, 'narrow')
- narrow_rowfactor: float32 [4, 8192], P(None, 'wide')
- narrow_colfactor: float32 [4, 1024], P(None, 'narrow')
The draws below stay inside these ranges and needn't reach their ends.
All inputs are finite; a program needn't handle non-finite values.
Results may differ from the reference program's by a relative error of at most 0.0004.
Values sent between devices are 32-bit elements; how exact they have to be, the bound alone decides.
A program may use at most 128 MiB of HBM per device.

```python
import jax
import jax.numpy as jnp
from jax import lax

MODEL_WIDTH = 8192
KEY_VALUE_WIDTH = 1024
NSQ = 4
KEY_VALUE_COUNT = 4


def scale_profile(key, count, length, reverse):
    place = jnp.arange(length, dtype=jnp.float32) / length
    if reverse:
        place = 1.0 - place
    jitter = jax.random.uniform(key, (count, length), jnp.float32)
    return 10.0 ** (0.5 * place[None, :] + 0.5 * jitter)


def gradient_sample(key, count, length, width):
    row_scale = scale_profile(jax.random.fold_in(key, 11), count, length, False)
    col_first = scale_profile(jax.random.fold_in(key, 12), count, width, False)
    col_second = scale_profile(jax.random.fold_in(key, 15), count, width, True)
    mixing = jax.random.uniform(jax.random.fold_in(key, 16), (count, length, 1), jnp.float32)
    col_mixed = jnp.sqrt(mixing * jnp.square(col_first)[:, None, :] + (1.0 - mixing) * jnp.square(col_second)[:, None, :])
    noise = jax.random.truncated_normal(jax.random.fold_in(key, 13), -4.0, 4.0, (count, length, width), jnp.float32)
    return (0.01 * noise * row_scale[:, :, None] * col_mixed).astype(jnp.bfloat16)


def state_sample(key, count, length):
    place = jnp.arange(length, dtype=jnp.float32) / length
    noise = 10.0 ** jax.random.uniform(key, (count, length), jnp.float32, -0.5, 0.5)
    return 0.002 * (10.0 ** place)[None, :] * noise


def level_sample(key, count):
    order = jax.random.permutation(key, count)
    level_values = 10.0 ** jnp.linspace(-1.5, 1.5, count, dtype=jnp.float32)
    return level_values[order]


def draw_square_grads(key, part):
    return gradient_sample(jax.random.fold_in(key, 1), NSQ, MODEL_WIDTH, MODEL_WIDTH)


def draw_narrow_grads(key, part):
    return gradient_sample(jax.random.fold_in(key, 2), KEY_VALUE_COUNT, MODEL_WIDTH, KEY_VALUE_WIDTH)


def draw_square_rowstate(key, part):
    return state_sample(jax.random.fold_in(key, 3), NSQ, MODEL_WIDTH)


def draw_narrow_rowstate(key, part):
    return state_sample(jax.random.fold_in(key, 4), KEY_VALUE_COUNT, MODEL_WIDTH)


def draw_square_colstate(key, part):
    level_values = level_sample(jax.random.fold_in(key, 5), NSQ)
    return state_sample(jax.random.fold_in(key, 6), NSQ, MODEL_WIDTH) * level_values[:, None]


def draw_narrow_colstate(key, part):
    level_values = level_sample(jax.random.fold_in(key, 7), KEY_VALUE_COUNT)
    return state_sample(jax.random.fold_in(key, 8), KEY_VALUE_COUNT, KEY_VALUE_WIDTH) * level_values[:, None]


def setup_inputs(seed: int = 0) -> dict:
    keys = jax.random.split(jax.random.key(seed), 7)
    square_grads = draw_square_grads(jax.random.fold_in(keys[6], 71), 0)
    narrow_grads = draw_narrow_grads(jax.random.fold_in(keys[6], 71), 0)
    square_rowstate = draw_square_rowstate(jax.random.fold_in(keys[6], 71), 0)
    square_colstate = draw_square_colstate(jax.random.fold_in(keys[6], 71), 0)
    narrow_rowstate = draw_narrow_rowstate(jax.random.fold_in(keys[6], 71), 0)
    narrow_colstate = draw_narrow_colstate(jax.random.fold_in(keys[6], 71), 0)
    return dict(square_grads=square_grads, narrow_grads=narrow_grads, square_rowstate=square_rowstate, square_colstate=square_colstate, narrow_rowstate=narrow_rowstate, narrow_colstate=narrow_colstate)


decay_rate = 0.9
epsilon_square = 1e-30
clip_limit = 1.0

def one_matrix(inputs):
    grads, rowstate, colstate = inputs
    values = grads.astype(jnp.float32)
    squares = values * values + epsilon_square
    rowfactor = decay_rate * rowstate + (1.0 - decay_rate) * lax.optimization_barrier(jnp.mean(squares, axis=1))
    colfactor = decay_rate * colstate + (1.0 - decay_rate) * lax.optimization_barrier(jnp.mean(squares, axis=0))
    row_mean = jnp.mean(rowfactor)
    raw = values * lax.rsqrt(rowfactor)[:, None] * lax.rsqrt(colfactor)[None, :] * jnp.sqrt(row_mean)
    spread = jnp.sqrt(jnp.mean(raw * raw))
    update = raw / jnp.maximum(1.0, spread / clip_limit)
    return (update, rowfactor, colfactor)

def reference(square_grads, narrow_grads, square_rowstate, square_colstate, narrow_rowstate, narrow_colstate):
    square_update, square_rowfactor, square_colfactor = lax.map(one_matrix, (square_grads, square_rowstate, square_colstate))
    narrow_update, narrow_rowfactor, narrow_colfactor = lax.map(one_matrix, (narrow_grads, narrow_rowstate, narrow_colstate))
    return (square_update, narrow_update, square_rowfactor, square_colfactor, narrow_rowfactor, narrow_colfactor)
```

```python
import functools

import jax
import jax.numpy as jnp
from jax import lax
from jax.experimental import pallas as pl
from jax.experimental.pallas import tpu as pltpu
from jax.sharding import PartitionSpec as P

decay_rate = 0.9
epsilon_square = 1e-30
clip_limit = 1.0
LANES = 128
AHEAD = 6


def square_sums(grads):
    values = grads.astype(jnp.float32)
    squares = values * values + epsilon_square
    return (values, jnp.sum(squares, axis=2), jnp.sum(squares, axis=1))


def blend(state, total, count):
    return decay_rate * state + (1.0 - decay_rate) * (total / count)


def scaled(values, rowfactor, colfactor, row_mean):
    return (
        values
        * lax.rsqrt(rowfactor)[:, :, None]
        * lax.rsqrt(colfactor)[:, None, :]
        * jnp.sqrt(row_mean)[:, None, None]
    )


def clipped(raw, norm, entries):
    spread = jnp.sqrt(norm / entries)
    return raw / jnp.maximum(1.0, spread / clip_limit)[:, None, None]


def plain_per_device(
    square_grads, narrow_grads, square_rowstate, square_colstate, narrow_rowstate, narrow_colstate
):
    total_rows = square_grads.shape[1] * lax.axis_size("wide")
    square_width = square_grads.shape[2] * lax.axis_size("narrow")
    narrow_width = narrow_grads.shape[2] * lax.axis_size("narrow")
    square_values, square_rowpart, square_colpart = square_sums(square_grads)
    narrow_values, narrow_rowpart, narrow_colpart = square_sums(narrow_grads)
    square_rowsum, narrow_rowsum = lax.psum((square_rowpart, narrow_rowpart), "narrow")
    square_colsum, narrow_colsum = lax.psum((square_colpart, narrow_colpart), "wide")
    square_rowfactor = blend(square_rowstate, square_rowsum, square_width)
    narrow_rowfactor = blend(narrow_rowstate, narrow_rowsum, narrow_width)
    square_colfactor = blend(square_colstate, square_colsum, total_rows)
    narrow_colfactor = blend(narrow_colstate, narrow_colsum, total_rows)
    square_rowtotal, narrow_rowtotal = lax.psum(
        (jnp.sum(square_rowfactor, axis=1), jnp.sum(narrow_rowfactor, axis=1)), "wide"
    )
    square_mean = square_rowtotal / total_rows
    narrow_mean = narrow_rowtotal / total_rows
    square_raw = scaled(square_values, square_rowfactor, square_colfactor, square_mean)
    narrow_raw = scaled(narrow_values, narrow_rowfactor, narrow_colfactor, narrow_mean)
    square_norm, narrow_norm = lax.psum(
        (
            jnp.sum(square_raw * square_raw, axis=(1, 2)),
            jnp.sum(narrow_raw * narrow_raw, axis=(1, 2)),
        ),
        ("wide", "narrow"),
    )
    square_update = clipped(square_raw, square_norm, total_rows * square_width)
    narrow_update = clipped(narrow_raw, narrow_norm, total_rows * narrow_width)
    return (
        square_update,
        narrow_update,
        square_rowfactor,
        square_colfactor,
        narrow_rowfactor,
        narrow_colfactor,
    )


def tiled(x, count):
    return jnp.concatenate([x] * count, axis=1) if count > 1 else x


def fold(values):
    out = values[0:8]
    for i in range(8, values.shape[0], 8):
        out = out + values[i : i + 8]
    return out


def picked_row(values, index):
    row = lax.broadcasted_iota(jnp.int32, values.shape, 0)
    return jnp.sum(jnp.where(row == index, values, 0.0), axis=0, keepdims=True)


def column_block(cols):
    block = 1024
    while cols % block:
        block //= 2
    return block


def stats_kernel(
    wide, narrow,
    sq_hbm, na_hbm, sq_rs, sq_cs, na_rs, na_cs,
    sq_rf, sq_cf, na_rf, na_cf, scale_out,
    sq_buf, na_buf, rowpart, rowinv, row_mine, row_theirs, col_mine, col_theirs, col_all,
    sq_w, na_w, table, finals,
    in_sems, row_send, row_recv, rs_send, rs_recv, ag_send, ag_recv, fin_send, fin_recv,
):
    count, rows, sq_cols = sq_hbm.shape
    na_cols = na_hbm.shape[2]
    total_rows = rows * wide
    me_w, me_n = lax.axis_index("wide"), lax.axis_index("narrow")
    me = me_w * narrow + me_n
    devices = wide * narrow
    step = 16
    mesh_id = pl.DeviceIdType.MESH

    def device(index):
        return (index // narrow, lax.rem(index, narrow))

    mats = []
    for m in range(count):
        mats.append((sq_hbm, sq_buf, sq_w, sq_rs, sq_rf, sq_cols, m, m))
        mats.append((na_hbm, na_buf, na_w, na_rs, na_rf, na_cols, m, count + m))

    chunks = []
    for hbm, buf, _, _, _, cols, m, _ in mats:
        block = column_block(cols)
        for start in range(0, cols, block):
            chunks.append((hbm, buf, m, start, block))
    copies = [
        pltpu.make_async_copy(
            hbm.at[m, :, pl.ds(start, block)], buf.at[m, :, pl.ds(start, block)], in_sems.at[i]
        )
        for i, (hbm, buf, m, start, block) in enumerate(chunks)
    ]
    for copy in copies[:AHEAD]:
        copy.start()

    barrier = pltpu.get_barrier_semaphore()

    @pl.loop(1, devices)
    def _(d):
        pl.semaphore_signal(
            barrier, inc=1, device_id=device(lax.rem(me + d, devices)), device_id_type=mesh_id
        )

    sq_per = sq_cols // LANES // wide
    na_blocks = na_cols // LANES
    na_per = count * na_blocks // wide

    def home(cols, m, block):
        if cols == sq_cols:
            return block // sq_per, m * sq_per + block % sq_per
        index = m * na_blocks + block
        return index // na_per, count * sq_per + index % na_per

    def row_copy(i):
        return pltpu.make_async_remote_copy(
            src_ref=row_mine.at[i],
            dst_ref=row_theirs.at[i],
            send_sem=row_send.at[i],
            recv_sem=row_recv.at[i],
            device_id=(me_w, 1 - me_n),
            device_id_type=mesh_id,
        )

    done = 0
    for order, (_, buf, _, _, _, cols, m, i) in enumerate(mats):
        block = column_block(cols)
        for start in range(0, cols, block):
            copies[done].wait()
            if done + AHEAD < len(copies):
                copies[done + AHEAD].start()
            done += 1

            def body(r, acc, buf=buf, m=m, start=start, block=block):
                at = pl.ds(pl.multiple_of(r * step, step), step)
                values = buf[m, at, pl.ds(start, block)].astype(jnp.float32)
                squares = values * values
                part = squares[:, 0:LANES]
                for k in range(LANES, block, LANES):
                    part = part + squares[:, k : k + LANES]
                if start:
                    part = part + rowpart[at, :]
                rowpart[at, :] = part
                return acc + fold(squares)

            acc = lax.fori_loop(
                0, rows // step, body, jnp.zeros((8, block), jnp.float32), unroll=2
            )
            sums = jnp.sum(acc, axis=0, keepdims=True)
            for b in range(block // LANES):
                owner, row = home(cols, m, start // LANES + b)
                col_mine[owner, row : row + 1, :] = sums[:, b * LANES : (b + 1) * LANES]
        for q in range(rows // LANES):
            square = rowpart[q * LANES : (q + 1) * LANES, :].T
            row_mine[i, q : q + 1, :] = jnp.sum(square, axis=0, keepdims=True)
        if order == 0:
            pl.semaphore_wait(barrier, devices - 1)
        row_copy(i).start()

    def rs_copy(d):
        peer = lax.rem(me_w + d, wide)
        return pltpu.make_async_remote_copy(
            src_ref=col_mine.at[peer],
            dst_ref=col_theirs.at[d],
            send_sem=rs_send.at[d],
            recv_sem=rs_recv.at[d],
            device_id=(peer, me_n),
            device_id_type=mesh_id,
        )

    @pl.loop(1, wide)
    def _(d):
        rs_copy(d).start()

    def ag_copy(d):
        peer = lax.rem(me_w + d, wide)
        return pltpu.make_async_remote_copy(
            src_ref=col_all.at[me_w],
            dst_ref=col_all.at[me_w],
            send_sem=ag_send.at[d],
            recv_sem=ag_recv.at[me_w],
            device_id=(peer, me_n),
            device_id_type=mesh_id,
        )

    def own_columns():
        @pl.loop(1, wide)
        def _(d):
            rs_copy(d).wait_recv()

        total = col_mine[me_w]
        for d in range(1, wide):
            total = total + col_theirs[d]

        def put(row, state):
            mean = total[row : row + 1] / total_rows + epsilon_square
            col_all[me_w, row : row + 1, :] = decay_rate * state + (1.0 - decay_rate) * mean

        for m in range(count):
            for b in range(sq_per):
                at = pl.multiple_of((me_w * sq_per + b) * LANES, LANES)
                put(m * sq_per + b, sq_cs[m : m + 1, pl.ds(at, LANES)])
        for b in range(na_per):
            index = me_w * na_per + b
            at = pl.multiple_of(lax.rem(index, na_blocks) * LANES, LANES)
            put(count * sq_per + b, picked_row(na_cs[:, pl.ds(at, LANES)], index // na_blocks))

        @pl.loop(1, wide)
        def _(d):
            ag_copy(d).start()

    for order, (_, buf, w, rs, rf, cols, m, i) in enumerate(mats):
        if order == 5:
            own_columns()
        row_copy(i).wait_recv()
        width = cols * narrow
        factors = jnp.zeros((1, LANES), jnp.float32)
        for q in range(rows // LANES):
            lanes = slice(q * LANES, (q + 1) * LANES)
            mean = (row_mine[i, q : q + 1, :] + row_theirs[i, q : q + 1, :]) / width
            factor = decay_rate * rs[m : m + 1, lanes] + (1.0 - decay_rate) * (
                mean + epsilon_square
            )
            rf[m : m + 1, lanes] = factor
            factors = factors + factor
            root = lax.rsqrt(factor)
            rowinv[lanes, :] = jnp.broadcast_to(root * root, (LANES, LANES)).T
        table[2 * count + i : 2 * count + i + 1, :] = factors
        block = column_block(cols)
        for start in range(0, cols, block):

            def body(r, acc, buf=buf, m=m, start=start, block=block):
                at = pl.ds(pl.multiple_of(r * step, step), step)
                values = buf[m, at, pl.ds(start, block)].astype(jnp.float32)
                inv = tiled(rowinv[at, :], block // LANES)
                return acc + fold(values * values * inv)

            w[m, :, start : start + block] = lax.fori_loop(
                0, rows // step, body, jnp.zeros((8, block), jnp.float32), unroll=2
            )

    @pl.loop(1, wide)
    def _(d):
        source = lax.rem(me_w + d, wide)
        pltpu.make_async_remote_copy(
            src_ref=col_all.at[source],
            dst_ref=col_all.at[source],
            send_sem=ag_send.at[d],
            recv_sem=ag_recv.at[source],
            device_id=(source, me_n),
            device_id_type=mesh_id,
        ).wait_recv()

    for _, _, w, _, _, cols, m, i in mats:
        cf = sq_cf if cols == sq_cols else na_cf
        part = jnp.zeros((8, LANES), jnp.float32)
        for b in range(cols // LANES):
            owner, row = home(cols, m, b)
            lanes = slice(b * LANES, (b + 1) * LANES)
            factor = col_all[owner, row : row + 1, :]
            cf[m : m + 1, lanes] = factor
            root = lax.rsqrt(factor)
            part = part + w[m, :, lanes] * (root * root)
        table[i : i + 1, :] = jnp.sum(part, axis=0, keepdims=True)

    height = 4 * count
    lane = lax.broadcasted_iota(jnp.int32, (height, LANES), 1)
    sub = lax.broadcasted_iota(jnp.int32, (height, LANES), 0)
    sums = jnp.sum(table[...], axis=1, keepdims=True)
    finals[me] = jnp.sum(jnp.where(lane == sub, sums, 0.0), axis=0, keepdims=True)

    def fin_copy(slot, d, peer):
        return pltpu.make_async_remote_copy(
            src_ref=finals.at[slot],
            dst_ref=finals.at[slot],
            send_sem=fin_send.at[d],
            recv_sem=fin_recv.at[slot],
            device_id=device(peer),
            device_id_type=mesh_id,
        )

    @pl.loop(1, devices)
    def _(d):
        fin_copy(me, d, lax.rem(me + d, devices)).start()

    for i in range(2 * count):
        row_copy(i).wait_send()

    @pl.loop(1, wide)
    def _(d):
        rs_copy(d).wait_send()
        ag_copy(d).wait_send()

    @pl.loop(1, devices)
    def _(d):
        source = lax.rem(me + d, devices)
        fin_copy(source, d, source).wait_recv()

    total = finals[0]
    for k in range(1, devices):
        total = total + finals[k]
    mean = pltpu.roll(total, LANES - 2 * count, axis=1) / (total_rows * narrow)
    place = lax.broadcasted_iota(jnp.int32, (1, LANES), 1)
    entries = jnp.where(
        place < count, float(total_rows * sq_cols * narrow), float(total_rows * na_cols * narrow)
    )
    spread = jnp.sqrt(mean * total / entries)
    scale = jnp.sqrt(mean) / jnp.maximum(1.0, spread / clip_limit)
    lane = lax.broadcasted_iota(jnp.int32, (2 * count, LANES), 1)
    sub = lax.broadcasted_iota(jnp.int32, (2 * count, LANES), 0)
    picked = jnp.sum(jnp.where(lane == sub, scale, 0.0), axis=1, keepdims=True)
    scale_out[...] = jnp.broadcast_to(picked, (2 * count, LANES))

    @pl.loop(1, devices)
    def _(d):
        fin_copy(me, d, lax.rem(me + d, devices)).wait_send()


def update_kernel(
    count,
    sq_g, na_g, sq_rf, sq_cf, na_rf, na_cf, scale,
    sq_out, na_out, sq_rf_out, sq_cf_out, na_rf_out, na_cf_out,
):
    m, q = pl.program_id(0), pl.program_id(1)
    at = pl.multiple_of(q * LANES, LANES)

    @pl.when((m == 0) & (q == 0))
    def _():
        sq_rf_out[...] = sq_rf[...]
        sq_cf_out[...] = sq_cf[...]
        na_rf_out[...] = na_rf[...]
        na_cf_out[...] = na_cf[...]

    for g, rf, cf, out, first in (
        (sq_g, sq_rf, sq_cf, sq_out, 0),
        (na_g, na_rf, na_cf, na_out, count),
    ):
        rowmul = lax.rsqrt(picked_row(rf[:, pl.ds(at, LANES)], m)) * scale[pl.ds(first + m, 1), :]
        rowmul = jnp.broadcast_to(rowmul, (LANES, LANES)).T
        cols = g.shape[2]
        block = min(cols, 512)
        for start in range(0, cols, block):
            colmul = lax.rsqrt(cf[pl.ds(m, 1), pl.ds(start, block)])
            values = g[0, :, pl.ds(start, block)].astype(jnp.float32)
            out[0, :, pl.ds(start, block)] = values * tiled(rowmul, block // LANES) * colmul


def kernel_per_device(wide, narrow, square_grads, narrow_grads, *states):
    count, rows, sq_cols = square_grads.shape
    na_cols = narrow_grads.shape[2]
    f32 = jnp.float32
    vmem = pl.BlockSpec(memory_space=pltpu.VMEM)
    hbm = pl.BlockSpec(memory_space=pl.ANY)
    shape = jax.ShapeDtypeStruct
    table_rows = count * (sq_cols + na_cols) // LANES // wide
    chunks = count * (sq_cols // column_block(sq_cols) + na_cols // column_block(na_cols))
    dma = pltpu.SemaphoreType.DMA
    factors = (
        shape((count, rows), f32),
        shape((count, sq_cols), f32),
        shape((count, rows), f32),
        shape((count, na_cols), f32),
    )
    stats = pl.pallas_call(
        functools.partial(stats_kernel, wide, narrow),
        out_shape=factors + (shape((2 * count, LANES), f32),),
        in_specs=[hbm, hbm, vmem, vmem, vmem, vmem],
        out_specs=[vmem] * 5,
        scratch_shapes=[
            pltpu.VMEM((count, rows, sq_cols), square_grads.dtype),
            pltpu.VMEM((count, rows, na_cols), narrow_grads.dtype),
            pltpu.VMEM((rows, LANES), f32),
            pltpu.VMEM((rows, LANES), f32),
            pltpu.VMEM((2 * count, rows // LANES, LANES), f32),
            pltpu.VMEM((2 * count, rows // LANES, LANES), f32),
            pltpu.VMEM((wide, table_rows, LANES), f32),
            pltpu.VMEM((wide, table_rows, LANES), f32),
            pltpu.VMEM((wide, table_rows, LANES), f32),
            pltpu.VMEM((count, 8, sq_cols), f32),
            pltpu.VMEM((count, 8, na_cols), f32),
            pltpu.VMEM((4 * count, LANES), f32),
            pltpu.VMEM((wide * narrow, 1, LANES), f32),
            dma((chunks,)),
            dma((2 * count,)),
            dma((2 * count,)),
            dma((wide,)),
            dma((wide,)),
            dma((wide,)),
            dma((wide,)),
            dma((wide * narrow,)),
            dma((wide * narrow,)),
        ],
        compiler_params=pltpu.CompilerParams(
            collective_id=0, has_side_effects=True, vmem_limit_bytes=40 * 2**20
        ),
        name="stats",
    )(square_grads, narrow_grads, *states)

    full = lambda s: pl.BlockSpec(s.shape, lambda m, q: (0, 0))
    blocked = lambda cols: pl.BlockSpec((1, LANES, cols), lambda m, q: (m, q, 0))
    square_update, narrow_update, *small = pl.pallas_call(
        functools.partial(update_kernel, count),
        grid=(count, rows // LANES),
        out_shape=(
            shape(square_grads.shape, f32),
            shape(narrow_grads.shape, f32),
        )
        + factors,
        in_specs=[blocked(sq_cols), blocked(na_cols)]
        + [full(s) for s in factors]
        + [pl.BlockSpec((2 * count, LANES), lambda m, q: (0, 0))],
        out_specs=[blocked(sq_cols), blocked(na_cols)] + [full(s) for s in factors],
        compiler_params=pltpu.CompilerParams(
            dimension_semantics=("arbitrary", "arbitrary"), vmem_limit_bytes=20 * 2**20
        ),
        name="update",
    )(square_grads, narrow_grads, *stats)
    return (square_update, narrow_update, *small)


def solution(mesh):
    wide, narrow = mesh.shape["wide"], mesh.shape["narrow"]

    def per_device(square_grads, narrow_grads, *states):
        count, rows, sq_cols = square_grads.shape
        na_cols = narrow_grads.shape[2]
        whole_tiles = (
            narrow == 2
            and wide > 1
            and rows % LANES == 0
            and sq_cols % (LANES * wide) == 0
            and na_cols % LANES == 0
            and sq_cols != na_cols
            and (count * na_cols) % (LANES * wide) == 0
            and 4 * count <= LANES
        )
        if whole_tiles:
            return kernel_per_device(wide, narrow, square_grads, narrow_grads, *states)
        return plain_per_device(square_grads, narrow_grads, *states)

    placed = (
        P(None, "wide", "narrow"),
        P(None, "wide", "narrow"),
        P(None, "wide"),
        P(None, "narrow"),
        P(None, "wide"),
        P(None, "narrow"),
    )
    return jax.shard_map(
        per_device,
        mesh=mesh,
        in_specs=placed,
        out_specs=placed,
        check_vma=False,
    )
```

```python
import functools

import jax
import jax.numpy as jnp
from jax import lax
from jax.experimental import pallas as pl
from jax.experimental.pallas import tpu as pltpu
from jax.sharding import PartitionSpec as P

decay_rate = 0.9
epsilon_square = 1e-30
clip_limit = 1.0
LANES = 128
AHEAD = 6


def square_sums(grads):
    values = grads.astype(jnp.float32)
    squares = values * values + epsilon_square
    return (values, jnp.sum(squares, axis=2), jnp.sum(squares, axis=1))


def blend(state, total, count):
    return decay_rate * state + (1.0 - decay_rate) * (total / count)


def scaled(values, rowfactor, colfactor, row_mean):
    return (
        values
        * lax.rsqrt(rowfactor)[:, :, None]
        * lax.rsqrt(colfactor)[:, None, :]
        * jnp.sqrt(row_mean)[:, None, None]
    )


def clipped(raw, norm, entries):
    spread = jnp.sqrt(norm / entries)
    return raw / jnp.maximum(1.0, spread / clip_limit)[:, None, None]


def plain_per_device(
    square_grads, narrow_grads, square_rowstate, square_colstate, narrow_rowstate, narrow_colstate
):
    total_rows = square_grads.shape[1] * lax.axis_size("wide")
    square_width = square_grads.shape[2] * lax.axis_size("narrow")
    narrow_width = narrow_grads.shape[2] * lax.axis_size("narrow")
    square_values, square_rowpart, square_colpart = square_sums(square_grads)
    narrow_values, narrow_rowpart, narrow_colpart = square_sums(narrow_grads)
    square_rowsum, narrow_rowsum = lax.psum((square_rowpart, narrow_rowpart), "narrow")
    square_colsum, narrow_colsum = lax.psum((square_colpart, narrow_colpart), "wide")
    square_rowfactor = blend(square_rowstate, square_rowsum, square_width)
    narrow_rowfactor = blend(narrow_rowstate, narrow_rowsum, narrow_width)
    square_colfactor = blend(square_colstate, square_colsum, total_rows)
    narrow_colfactor = blend(narrow_colstate, narrow_colsum, total_rows)
    square_rowtotal, narrow_rowtotal = lax.psum(
        (jnp.sum(square_rowfactor, axis=1), jnp.sum(narrow_rowfactor, axis=1)), "wide"
    )
    square_mean = square_rowtotal / total_rows
    narrow_mean = narrow_rowtotal / total_rows
    square_raw = scaled(square_values, square_rowfactor, square_colfactor, square_mean)
    narrow_raw = scaled(narrow_values, narrow_rowfactor, narrow_colfactor, narrow_mean)
    square_norm, narrow_norm = lax.psum(
        (
            jnp.sum(square_raw * square_raw, axis=(1, 2)),
            jnp.sum(narrow_raw * narrow_raw, axis=(1, 2)),
        ),
        ("wide", "narrow"),
    )
    square_update = clipped(square_raw, square_norm, total_rows * square_width)
    narrow_update = clipped(narrow_raw, narrow_norm, total_rows * narrow_width)
    return (
        square_update,
        narrow_update,
        square_rowfactor,
        square_colfactor,
        narrow_rowfactor,
        narrow_colfactor,
    )


def tiled(x, count):
    return jnp.concatenate([x] * count, axis=1) if count > 1 else x


def fold(values):
    out = values[0:8]
    for i in range(8, values.shape[0], 8):
        out = out + values[i : i + 8]
    return out


def picked_row(values, index):
    row = lax.broadcasted_iota(jnp.int32, values.shape, 0)
    return jnp.sum(jnp.where(row == index, values, 0.0), axis=0, keepdims=True)


def column_block(cols):
    block = 1024
    while cols % block:
        block //= 2
    return block


def stats_kernel(
    wide, narrow,
    sq_hbm, na_hbm, sq_rs_hbm, sq_cs_hbm, na_rs_hbm, na_cs_hbm,
    sq_rf, sq_cf, na_rf, na_cf, scale_out, sq_buf, na_buf,
    sq_rs, sq_cs, na_rs, na_cs, rowpart, rowinv, row_mine, row_theirs, col_mine, col_theirs, col_all,
    sq_w, na_w, table, finals,
    in_sems, state_sems, row_send, row_recv, rs_send, rs_recv, ag_send, ag_recv, fin_send, fin_recv,
):
    count, rows, sq_cols = sq_hbm.shape
    na_cols = na_hbm.shape[2]
    total_rows = rows * wide
    me_w, me_n = lax.axis_index("wide"), lax.axis_index("narrow")
    me = me_w * narrow + me_n
    devices = wide * narrow
    step = 16
    mesh_id = pl.DeviceIdType.MESH

    def device(index):
        return (index // narrow, lax.rem(index, narrow))

    mats = []
    for m in range(count):
        mats.append((sq_hbm, sq_buf, sq_w, sq_rs, sq_rf, sq_cols, m, m))
        mats.append((na_hbm, na_buf, na_w, na_rs, na_rf, na_cols, m, count + m))

    chunks = []
    for hbm, buf, _, _, _, cols, m, _ in mats:
        block = column_block(cols)
        for start in range(0, cols, block):
            chunks.append((hbm, buf, m, start, block))
    copies = [
        pltpu.make_async_copy(
            hbm.at[m, :, pl.ds(start, block)], buf.at[m, :, pl.ds(start, block)], in_sems.at[i]
        )
        for i, (hbm, buf, m, start, block) in enumerate(chunks)
    ]
    states = [
        pltpu.make_async_copy(src, dst, state_sems.at[i])
        for i, (src, dst) in enumerate(
            ((sq_rs_hbm, sq_rs), (sq_cs_hbm, sq_cs), (na_rs_hbm, na_rs), (na_cs_hbm, na_cs))
        )
    ]
    for copy in copies[:AHEAD] + states:
        copy.start()

    barrier = pltpu.get_barrier_semaphore()

    @pl.loop(1, devices)
    def _(d):
        pl.semaphore_signal(
            barrier, inc=1, device_id=device(lax.rem(me + d, devices)), device_id_type=mesh_id
        )

    sq_per = sq_cols // LANES // wide
    na_blocks = na_cols // LANES
    na_per = count * na_blocks // wide

    def home(cols, m, block):
        if cols == sq_cols:
            return block // sq_per, m * sq_per + block % sq_per
        index = m * na_blocks + block
        return index // na_per, count * sq_per + index % na_per

    def row_copy(i):
        return pltpu.make_async_remote_copy(
            src_ref=row_mine.at[i],
            dst_ref=row_theirs.at[i],
            send_sem=row_send.at[i],
            recv_sem=row_recv.at[i],
            device_id=(me_w, 1 - me_n),
            device_id_type=mesh_id,
        )

    done = 0
    for order, (_, buf, _, _, _, cols, m, i) in enumerate(mats):
        block = column_block(cols)
        for start in range(0, cols, block):
            copies[done].wait()
            if done + AHEAD < len(copies):
                copies[done + AHEAD].start()
            done += 1

            def body(r, acc, buf=buf, m=m, start=start, block=block):
                at = pl.ds(pl.multiple_of(r * step, step), step)
                values = buf[m, at, pl.ds(start, block)].astype(jnp.float32)
                squares = values * values
                part = squares[:, 0:LANES]
                for k in range(LANES, block, LANES):
                    part = part + squares[:, k : k + LANES]
                if start:
                    part = part + rowpart[at, :]
                rowpart[at, :] = part
                return acc + fold(squares)

            acc = lax.fori_loop(
                0, rows // step, body, jnp.zeros((8, block), jnp.float32), unroll=2
            )
            sums = jnp.sum(acc, axis=0, keepdims=True)
            for b in range(block // LANES):
                owner, row = home(cols, m, start // LANES + b)
                col_mine[owner, row : row + 1, :] = sums[:, b * LANES : (b + 1) * LANES]
        for q in range(rows // LANES):
            square = rowpart[q * LANES : (q + 1) * LANES, :].T
            row_mine[i, q : q + 1, :] = jnp.sum(square, axis=0, keepdims=True)
        if order == 0:
            pl.semaphore_wait(barrier, devices - 1)
        row_copy(i).start()

    def rs_copy(d):
        peer = lax.rem(me_w + d, wide)
        return pltpu.make_async_remote_copy(
            src_ref=col_mine.at[peer],
            dst_ref=col_theirs.at[d],
            send_sem=rs_send.at[d],
            recv_sem=rs_recv.at[d],
            device_id=(peer, me_n),
            device_id_type=mesh_id,
        )

    @pl.loop(1, wide)
    def _(d):
        rs_copy(d).start()

    for copy in states:
        copy.wait()

    def ag_copy(d):
        peer = lax.rem(me_w + d, wide)
        return pltpu.make_async_remote_copy(
            src_ref=col_all.at[me_w],
            dst_ref=col_all.at[me_w],
            send_sem=ag_send.at[d],
            recv_sem=ag_recv.at[me_w],
            device_id=(peer, me_n),
            device_id_type=mesh_id,
        )

    def own_columns():
        @pl.loop(1, wide)
        def _(d):
            rs_copy(d).wait_recv()

        total = col_mine[me_w]
        for d in range(1, wide):
            total = total + col_theirs[d]

        def put(row, state):
            mean = total[row : row + 1] / total_rows + epsilon_square
            col_all[me_w, row : row + 1, :] = decay_rate * state + (1.0 - decay_rate) * mean

        for m in range(count):
            for b in range(sq_per):
                at = pl.multiple_of((me_w * sq_per + b) * LANES, LANES)
                put(m * sq_per + b, sq_cs[m : m + 1, pl.ds(at, LANES)])
        for b in range(na_per):
            index = me_w * na_per + b
            at = pl.multiple_of(lax.rem(index, na_blocks) * LANES, LANES)
            put(count * sq_per + b, picked_row(na_cs[:, pl.ds(at, LANES)], index // na_blocks))

        @pl.loop(1, wide)
        def _(d):
            ag_copy(d).start()

    for order, (_, buf, w, rs, rf, cols, m, i) in enumerate(mats):
        if order == 5:
            own_columns()
        row_copy(i).wait_recv()
        width = cols * narrow
        factors = jnp.zeros((1, LANES), jnp.float32)
        for q in range(rows // LANES):
            lanes = slice(q * LANES, (q + 1) * LANES)
            mean = (row_mine[i, q : q + 1, :] + row_theirs[i, q : q + 1, :]) / width
            factor = decay_rate * rs[m : m + 1, lanes] + (1.0 - decay_rate) * (
                mean + epsilon_square
            )
            rf[m : m + 1, lanes] = factor
            factors = factors + factor
            root = lax.rsqrt(factor)
            rowinv[lanes, :] = jnp.broadcast_to(root * root, (LANES, LANES)).T
        table[2 * count + i : 2 * count + i + 1, :] = factors
        block = column_block(cols)
        for start in range(0, cols, block):

            def body(r, acc, buf=buf, m=m, start=start, block=block):
                at = pl.ds(pl.multiple_of(r * step, step), step)
                values = buf[m, at, pl.ds(start, block)].astype(jnp.float32)
                inv = tiled(rowinv[at, :], block // LANES)
                return acc + fold(values * values * inv)

            w[m, :, start : start + block] = lax.fori_loop(
                0, rows // step, body, jnp.zeros((8, block), jnp.float32), unroll=2
            )

    @pl.loop(1, wide)
    def _(d):
        source = lax.rem(me_w + d, wide)
        pltpu.make_async_remote_copy(
            src_ref=col_all.at[source],
            dst_ref=col_all.at[source],
            send_sem=ag_send.at[d],
            recv_sem=ag_recv.at[source],
            device_id=(source, me_n),
            device_id_type=mesh_id,
        ).wait_recv()

    for _, _, w, _, _, cols, m, i in mats:
        cf = sq_cf if cols == sq_cols else na_cf
        part = jnp.zeros((8, LANES), jnp.float32)
        for b in range(cols // LANES):
            owner, row = home(cols, m, b)
            lanes = slice(b * LANES, (b + 1) * LANES)
            factor = col_all[owner, row : row + 1, :]
            cf[m : m + 1, lanes] = factor
            root = lax.rsqrt(factor)
            part = part + w[m, :, lanes] * (root * root)
        table[i : i + 1, :] = jnp.sum(part, axis=0, keepdims=True)

    height = 4 * count
    lane = lax.broadcasted_iota(jnp.int32, (height, LANES), 1)
    sub = lax.broadcasted_iota(jnp.int32, (height, LANES), 0)
    sums = jnp.sum(table[...], axis=1, keepdims=True)
    finals[me] = jnp.sum(jnp.where(lane == sub, sums, 0.0), axis=0, keepdims=True)

    def fin_copy(slot, d, peer):
        return pltpu.make_async_remote_copy(
            src_ref=finals.at[slot],
            dst_ref=finals.at[slot],
            send_sem=fin_send.at[d],
            recv_sem=fin_recv.at[slot],
            device_id=device(peer),
            device_id_type=mesh_id,
        )

    @pl.loop(1, devices)
    def _(d):
        fin_copy(me, d, lax.rem(me + d, devices)).start()

    for i in range(2 * count):
        row_copy(i).wait_send()

    @pl.loop(1, wide)
    def _(d):
        rs_copy(d).wait_send()
        ag_copy(d).wait_send()

    @pl.loop(1, devices)
    def _(d):
        source = lax.rem(me + d, devices)
        fin_copy(source, d, source).wait_recv()

    total = finals[0]
    for k in range(1, devices):
        total = total + finals[k]
    mean = pltpu.roll(total, LANES - 2 * count, axis=1) / (total_rows * narrow)
    place = lax.broadcasted_iota(jnp.int32, (1, LANES), 1)
    entries = jnp.where(
        place < count, float(total_rows * sq_cols * narrow), float(total_rows * na_cols * narrow)
    )
    spread = jnp.sqrt(mean * total / entries)
    scale = jnp.sqrt(mean) / jnp.maximum(1.0, spread / clip_limit)
    lane = lax.broadcasted_iota(jnp.int32, (2 * count, LANES), 1)
    sub = lax.broadcasted_iota(jnp.int32, (2 * count, LANES), 0)
    picked = jnp.sum(jnp.where(lane == sub, scale, 0.0), axis=1, keepdims=True)
    scale_out[...] = jnp.broadcast_to(picked, (2 * count, LANES))

    @pl.loop(1, devices)
    def _(d):
        fin_copy(me, d, lax.rem(me + d, devices)).wait_send()


def update_kernel(
    sq_g, na_g, sq_rf, sq_cf, na_rf, na_cf, scale,
    sq_out, na_out, sq_rf_out, sq_cf_out, na_rf_out, na_cf_out,
    sq_slots, na_slots, sq_sems, na_sems, small_sems,
):
    count, rows, sq_cols = sq_g.shape
    slots = sq_slots.shape[0]
    per = rows // LANES
    half = LANES // 2
    small = [
        pltpu.make_async_copy(src, dst, small_sems.at[i])
        for i, (src, dst) in enumerate(
            ((sq_rf, sq_rf_out), (sq_cf, sq_cf_out), (na_rf, na_rf_out), (na_cf, na_cf_out))
        )
    ]
    for copy in small:
        copy.start()
    kinds = (
        (sq_g, sq_rf, sq_cf, sq_out, sq_slots, sq_sems, 0),
        (na_g, na_rf, na_cf, na_out, na_slots, na_sems, count),
    )

    def out_copy(kind, t, h):
        _, _, _, out, held, sems, _ = kind
        slot = lax.rem(t, slots)
        row = pl.multiple_of(lax.rem(t, per) * LANES + h * half, half)
        return pltpu.make_async_copy(
            held.at[slot, pl.ds(h * half, half), :],
            out.at[lax.div(t, per), pl.ds(row, half), :],
            sems.at[slot, h],
        )

    def wait(t):
        for kind in kinds:
            for h in range(2):
                out_copy(kind, t, h).wait()

    @pl.loop(0, count * per)
    def _(t):
        m, q, slot = lax.div(t, per), lax.rem(t, per), lax.rem(t, slots)
        at = pl.multiple_of(q * LANES, LANES)

        @pl.when(t >= slots)
        def _():
            wait(t - slots)

        for kind in kinds:
            g, rf, cf, _, held, _, first = kind
            rowmul = lax.rsqrt(picked_row(rf[:, pl.ds(at, LANES)], m)) * scale[pl.ds(first + m, 1), :]
            rowmul = jnp.broadcast_to(rowmul, (LANES, LANES)).T
            cols = g.shape[2]
            block = min(cols, 512)
            for h in range(2):
                rows_at = pl.ds(pl.multiple_of(at + h * half, half), half)
                mul = rowmul[h * half : (h + 1) * half]
                for start in range(0, cols, block):
                    colmul = lax.rsqrt(cf[pl.ds(m, 1), pl.ds(start, block)])
                    values = g[m, rows_at, pl.ds(start, block)].astype(jnp.float32)
                    held[slot, pl.ds(h * half, half), pl.ds(start, block)] = (
                        values * tiled(mul, block // LANES) * colmul
                    )
                out_copy(kind, t, h).start()

    for t in range(max(count * per - slots, 0), count * per):
        wait(t)
    for copy in small:
        copy.wait()


def kernel_per_device(wide, narrow, square_grads, narrow_grads, *states):
    count, rows, sq_cols = square_grads.shape
    na_cols = narrow_grads.shape[2]
    f32 = jnp.float32
    vmem = pl.BlockSpec(memory_space=pltpu.VMEM)
    hbm = pl.BlockSpec(memory_space=pltpu.HBM)
    shape = jax.ShapeDtypeStruct
    table_rows = count * (sq_cols + na_cols) // LANES // wide
    chunks = count * (sq_cols // column_block(sq_cols) + na_cols // column_block(na_cols))
    dma = pltpu.SemaphoreType.DMA
    slots = 3
    factors = (
        shape((count, rows), f32),
        shape((count, sq_cols), f32),
        shape((count, rows), f32),
        shape((count, na_cols), f32),
    )
    *stats, square_held, narrow_held = pl.pallas_call(
        functools.partial(stats_kernel, wide, narrow),
        out_shape=factors
        + (
            shape((2 * count, LANES), f32),
            shape(square_grads.shape, square_grads.dtype),
            shape(narrow_grads.shape, narrow_grads.dtype),
        ),
        in_specs=[hbm] * 6,
        out_specs=[vmem] * 7,
        scratch_shapes=[
            pltpu.VMEM((count, rows), f32),
            pltpu.VMEM((count, sq_cols), f32),
            pltpu.VMEM((count, rows), f32),
            pltpu.VMEM((count, na_cols), f32),
            pltpu.VMEM((rows, LANES), f32),
            pltpu.VMEM((rows, LANES), f32),
            pltpu.VMEM((2 * count, rows // LANES, LANES), f32),
            pltpu.VMEM((2 * count, rows // LANES, LANES), f32),
            pltpu.VMEM((wide, table_rows, LANES), f32),
            pltpu.VMEM((wide, table_rows, LANES), f32),
            pltpu.VMEM((wide, table_rows, LANES), f32),
            pltpu.VMEM((count, 8, sq_cols), f32),
            pltpu.VMEM((count, 8, na_cols), f32),
            pltpu.VMEM((4 * count, LANES), f32),
            pltpu.VMEM((wide * narrow, 1, LANES), f32),
            dma((chunks,)),
            dma((4,)),
            dma((2 * count,)),
            dma((2 * count,)),
            dma((wide,)),
            dma((wide,)),
            dma((wide,)),
            dma((wide,)),
            dma((wide * narrow,)),
            dma((wide * narrow,)),
        ],
        compiler_params=pltpu.CompilerParams(
            collective_id=0, has_side_effects=True, vmem_limit_bytes=12 * 2**20
        ),
        name="stats",
    )(*(pltpu.with_memory_space_constraint(x, pltpu.HBM) for x in (square_grads, narrow_grads, *states)))

    return pl.pallas_call(
        update_kernel,
        out_shape=(
            shape(square_grads.shape, f32),
            shape(narrow_grads.shape, f32),
        )
        + factors,
        in_specs=[vmem] * 7,
        out_specs=[hbm] * 6,
        scratch_shapes=[
            pltpu.VMEM((slots, LANES, sq_cols), f32),
            pltpu.VMEM((slots, LANES, na_cols), f32),
            dma((slots, 2)),
            dma((slots, 2)),
            dma((4,)),
        ],
        compiler_params=pltpu.CompilerParams(vmem_limit_bytes=12 * 2**20),
        name="update",
    )(square_held, narrow_held, *stats)


def solution(mesh):
    wide, narrow = mesh.shape["wide"], mesh.shape["narrow"]

    def per_device(square_grads, narrow_grads, *states):
        count, rows, sq_cols = square_grads.shape
        na_cols = narrow_grads.shape[2]
        whole_tiles = (
            narrow == 2
            and wide > 1
            and rows % LANES == 0
            and sq_cols % (LANES * wide) == 0
            and na_cols % LANES == 0
            and sq_cols != na_cols
            and (count * na_cols) % (LANES * wide) == 0
            and 4 * count <= LANES
        )
        if whole_tiles:
            return kernel_per_device(wide, narrow, square_grads, narrow_grads, *states)
        return plain_per_device(square_grads, narrow_grads, *states)

    placed = (
        P(None, "wide", "narrow"),
        P(None, "wide", "narrow"),
        P(None, "wide"),
        P(None, "narrow"),
        P(None, "wide"),
        P(None, "narrow"),
    )
    return jax.shard_map(
        per_device,
        mesh=mesh,
        in_specs=placed,
        out_specs=placed,
        check_vma=False,
    )
```

```python
import functools

import jax
import jax.numpy as jnp
from jax import lax
from jax.experimental import pallas as pl
from jax.experimental.pallas import tpu as pltpu
from jax.sharding import PartitionSpec as P

decay_rate = 0.9
epsilon_square = 1e-30
clip_limit = 1.0
LANES = 128
AHEAD = 8


def square_sums(grads):
    values = grads.astype(jnp.float32)
    squares = values * values + epsilon_square
    return (values, jnp.sum(squares, axis=2), jnp.sum(squares, axis=1))


def blend(state, total, count):
    return decay_rate * state + (1.0 - decay_rate) * (total / count)


def scaled(values, rowfactor, colfactor, row_mean):
    return (
        values
        * lax.rsqrt(rowfactor)[:, :, None]
        * lax.rsqrt(colfactor)[:, None, :]
        * jnp.sqrt(row_mean)[:, None, None]
    )


def clipped(raw, norm, entries):
    spread = jnp.sqrt(norm / entries)
    return raw / jnp.maximum(1.0, spread / clip_limit)[:, None, None]


def plain_per_device(
    square_grads, narrow_grads, square_rowstate, square_colstate, narrow_rowstate, narrow_colstate
):
    total_rows = square_grads.shape[1] * lax.axis_size("wide")
    square_width = square_grads.shape[2] * lax.axis_size("narrow")
    narrow_width = narrow_grads.shape[2] * lax.axis_size("narrow")
    square_values, square_rowpart, square_colpart = square_sums(square_grads)
    narrow_values, narrow_rowpart, narrow_colpart = square_sums(narrow_grads)
    square_rowsum, narrow_rowsum = lax.psum((square_rowpart, narrow_rowpart), "narrow")
    square_colsum, narrow_colsum = lax.psum((square_colpart, narrow_colpart), "wide")
    square_rowfactor = blend(square_rowstate, square_rowsum, square_width)
    narrow_rowfactor = blend(narrow_rowstate, narrow_rowsum, narrow_width)
    square_colfactor = blend(square_colstate, square_colsum, total_rows)
    narrow_colfactor = blend(narrow_colstate, narrow_colsum, total_rows)
    square_rowtotal, narrow_rowtotal = lax.psum(
        (jnp.sum(square_rowfactor, axis=1), jnp.sum(narrow_rowfactor, axis=1)), "wide"
    )
    square_mean = square_rowtotal / total_rows
    narrow_mean = narrow_rowtotal / total_rows
    square_raw = scaled(square_values, square_rowfactor, square_colfactor, square_mean)
    narrow_raw = scaled(narrow_values, narrow_rowfactor, narrow_colfactor, narrow_mean)
    square_norm, narrow_norm = lax.psum(
        (
            jnp.sum(square_raw * square_raw, axis=(1, 2)),
            jnp.sum(narrow_raw * narrow_raw, axis=(1, 2)),
        ),
        ("wide", "narrow"),
    )
    square_update = clipped(square_raw, square_norm, total_rows * square_width)
    narrow_update = clipped(narrow_raw, narrow_norm, total_rows * narrow_width)
    return (
        square_update,
        narrow_update,
        square_rowfactor,
        square_colfactor,
        narrow_rowfactor,
        narrow_colfactor,
    )


def tiled(x, count):
    return jnp.concatenate([x] * count, axis=1) if count > 1 else x


def fold(values):
    out = values[0:8]
    for i in range(8, values.shape[0], 8):
        out = out + values[i : i + 8]
    return out


def picked_row(values, index):
    row = lax.broadcasted_iota(jnp.int32, values.shape, 0)
    return jnp.sum(jnp.where(row == index, values, 0.0), axis=0, keepdims=True)


def column_block(cols):
    block = 1024
    while cols % block:
        block //= 2
    return block


def stats_kernel(
    wide, narrow,
    sq_hbm, na_hbm, sq_rs_hbm, sq_cs_hbm, na_rs_hbm, na_cs_hbm,
    sq_rf, sq_cf, na_rf, na_cf, scale_out, sq_buf, na_buf,
    sq_rs, sq_cs, na_rs, na_cs, rowpart, rowinv, row_mine, row_theirs, col_mine, col_theirs, col_all,
    sq_w, na_w, table, finals,
    in_sems, state_sems, row_send, row_recv, rs_send, rs_recv, ag_send, ag_recv, fin_send, fin_recv,
):
    count, rows, sq_cols = sq_hbm.shape
    na_cols = na_hbm.shape[2]
    total_rows = rows * wide
    me_w, me_n = lax.axis_index("wide"), lax.axis_index("narrow")
    me = me_w * narrow + me_n
    devices = wide * narrow
    step = 16
    mesh_id = pl.DeviceIdType.MESH

    def device(index):
        return (index // narrow, lax.rem(index, narrow))

    mats = []
    for m in range(count):
        mats.append((sq_hbm, sq_buf, sq_w, sq_rs, sq_rf, sq_cols, m, m))
        mats.append((na_hbm, na_buf, na_w, na_rs, na_rf, na_cols, m, count + m))

    chunks = []
    for hbm, buf, _, _, _, cols, m, _ in mats:
        block = column_block(cols)
        for start in range(0, cols, block):
            chunks.append((hbm, buf, m, start, block))
    copies = [
        pltpu.make_async_copy(
            hbm.at[m, :, pl.ds(start, block)], buf.at[m, :, pl.ds(start, block)], in_sems.at[i]
        )
        for i, (hbm, buf, m, start, block) in enumerate(chunks)
    ]
    states = [
        pltpu.make_async_copy(src, dst, state_sems.at[i])
        for i, (src, dst) in enumerate(
            ((sq_rs_hbm, sq_rs), (sq_cs_hbm, sq_cs), (na_rs_hbm, na_rs), (na_cs_hbm, na_cs))
        )
    ]
    for copy in copies[:AHEAD] + states:
        copy.start()

    barrier = pltpu.get_barrier_semaphore()

    @pl.loop(1, devices)
    def _(d):
        pl.semaphore_signal(
            barrier, inc=1, device_id=device(lax.rem(me + d, devices)), device_id_type=mesh_id
        )

    sq_per = sq_cols // LANES // wide
    na_blocks = na_cols // LANES
    na_per = count * na_blocks // wide

    def home(cols, m, block):
        if cols == sq_cols:
            return block // sq_per, m * sq_per + block % sq_per
        index = m * na_blocks + block
        return index // na_per, count * sq_per + index % na_per

    def row_copy(i):
        return pltpu.make_async_remote_copy(
            src_ref=row_mine.at[i],
            dst_ref=row_theirs.at[i],
            send_sem=row_send.at[i],
            recv_sem=row_recv.at[i],
            device_id=(me_w, 1 - me_n),
            device_id_type=mesh_id,
        )

    done = 0
    for order, (_, buf, _, _, _, cols, m, i) in enumerate(mats):
        block = column_block(cols)
        for start in range(0, cols, block):
            copies[done].wait()
            if done + AHEAD < len(copies):
                copies[done + AHEAD].start()
            done += 1

            def body(r, acc, buf=buf, m=m, start=start, block=block):
                at = pl.ds(pl.multiple_of(r * step, step), step)
                values = buf[m, at, pl.ds(start, block)].astype(jnp.float32)
                squares = values * values
                part = squares[:, 0:LANES]
                for k in range(LANES, block, LANES):
                    part = part + squares[:, k : k + LANES]
                if start:
                    part = part + rowpart[at, :]
                rowpart[at, :] = part
                return acc + fold(squares)

            acc = lax.fori_loop(
                0, rows // step, body, jnp.zeros((8, block), jnp.float32), unroll=4
            )
            sums = jnp.sum(acc, axis=0, keepdims=True)
            for b in range(block // LANES):
                owner, row = home(cols, m, start // LANES + b)
                col_mine[owner, row : row + 1, :] = sums[:, b * LANES : (b + 1) * LANES]
        for q in range(rows // LANES):
            square = rowpart[q * LANES : (q + 1) * LANES, :].T
            row_mine[i, q : q + 1, :] = jnp.sum(square, axis=0, keepdims=True)
        if order == 0:
            pl.semaphore_wait(barrier, devices - 1)
        row_copy(i).start()

    def rs_copy(d):
        peer = lax.rem(me_w + d, wide)
        return pltpu.make_async_remote_copy(
            src_ref=col_mine.at[peer],
            dst_ref=col_theirs.at[d],
            send_sem=rs_send.at[d],
            recv_sem=rs_recv.at[d],
            device_id=(peer, me_n),
            device_id_type=mesh_id,
        )

    @pl.loop(1, wide)
    def _(d):
        rs_copy(d).start()

    for copy in states:
        copy.wait()

    def ag_copy(d):
        peer = lax.rem(me_w + d, wide)
        return pltpu.make_async_remote_copy(
            src_ref=col_all.at[me_w],
            dst_ref=col_all.at[me_w],
            send_sem=ag_send.at[d],
            recv_sem=ag_recv.at[me_w],
            device_id=(peer, me_n),
            device_id_type=mesh_id,
        )

    def own_columns():
        @pl.loop(1, wide)
        def _(d):
            rs_copy(d).wait_recv()

        total = col_mine[me_w]
        for d in range(1, wide):
            total = total + col_theirs[d]

        def put(row, state):
            mean = total[row : row + 1] / total_rows + epsilon_square
            col_all[me_w, row : row + 1, :] = decay_rate * state + (1.0 - decay_rate) * mean

        for m in range(count):
            for b in range(sq_per):
                at = pl.multiple_of((me_w * sq_per + b) * LANES, LANES)
                put(m * sq_per + b, sq_cs[m : m + 1, pl.ds(at, LANES)])
        for b in range(na_per):
            index = me_w * na_per + b
            at = pl.multiple_of(lax.rem(index, na_blocks) * LANES, LANES)
            put(count * sq_per + b, picked_row(na_cs[:, pl.ds(at, LANES)], index // na_blocks))

        @pl.loop(1, wide)
        def _(d):
            ag_copy(d).start()

    for order, (_, buf, w, rs, rf, cols, m, i) in enumerate(mats):
        if order == 5:
            own_columns()
        row_copy(i).wait_recv()
        width = cols * narrow
        factors = jnp.zeros((1, LANES), jnp.float32)
        for q in range(rows // LANES):
            lanes = slice(q * LANES, (q + 1) * LANES)
            mean = (row_mine[i, q : q + 1, :] + row_theirs[i, q : q + 1, :]) / width
            factor = decay_rate * rs[m : m + 1, lanes] + (1.0 - decay_rate) * (
                mean + epsilon_square
            )
            rf[m : m + 1, lanes] = factor
            factors = factors + factor
            root = lax.rsqrt(factor)
            rowinv[lanes, :] = jnp.broadcast_to(root * root, (LANES, LANES)).T
        table[2 * count + i : 2 * count + i + 1, :] = factors
        block = column_block(cols)
        for start in range(0, cols, block):

            def body(r, acc, buf=buf, m=m, start=start, block=block):
                at = pl.ds(pl.multiple_of(r * step, step), step)
                values = buf[m, at, pl.ds(start, block)].astype(jnp.float32)
                inv = tiled(rowinv[at, :], block // LANES)
                return acc + fold(values * values * inv)

            w[m, :, start : start + block] = lax.fori_loop(
                0, rows // step, body, jnp.zeros((8, block), jnp.float32), unroll=4
            )

    @pl.loop(1, wide)
    def _(d):
        source = lax.rem(me_w + d, wide)
        pltpu.make_async_remote_copy(
            src_ref=col_all.at[source],
            dst_ref=col_all.at[source],
            send_sem=ag_send.at[d],
            recv_sem=ag_recv.at[source],
            device_id=(source, me_n),
            device_id_type=mesh_id,
        ).wait_recv()

    for _, _, w, _, _, cols, m, i in mats:
        cf = sq_cf if cols == sq_cols else na_cf
        part = jnp.zeros((8, LANES), jnp.float32)
        for b in range(cols // LANES):
            owner, row = home(cols, m, b)
            lanes = slice(b * LANES, (b + 1) * LANES)
            factor = col_all[owner, row : row + 1, :]
            cf[m : m + 1, lanes] = factor
            root = lax.rsqrt(factor)
            part = part + w[m, :, lanes] * (root * root)
        table[i : i + 1, :] = jnp.sum(part, axis=0, keepdims=True)

    height = 4 * count
    lane = lax.broadcasted_iota(jnp.int32, (height, LANES), 1)
    sub = lax.broadcasted_iota(jnp.int32, (height, LANES), 0)
    sums = jnp.sum(table[...], axis=1, keepdims=True)
    finals[me] = jnp.sum(jnp.where(lane == sub, sums, 0.0), axis=0, keepdims=True)

    def fin_copy(slot, d, peer):
        return pltpu.make_async_remote_copy(
            src_ref=finals.at[slot],
            dst_ref=finals.at[slot],
            send_sem=fin_send.at[d],
            recv_sem=fin_recv.at[slot],
            device_id=device(peer),
            device_id_type=mesh_id,
        )

    @pl.loop(1, devices)
    def _(d):
        fin_copy(me, d, lax.rem(me + d, devices)).start()

    for i in range(2 * count):
        row_copy(i).wait_send()

    @pl.loop(1, wide)
    def _(d):
        rs_copy(d).wait_send()
        ag_copy(d).wait_send()

    @pl.loop(1, devices)
    def _(d):
        source = lax.rem(me + d, devices)
        fin_copy(source, d, source).wait_recv()

    total = finals[0]
    for k in range(1, devices):
        total = total + finals[k]
    mean = pltpu.roll(total, LANES - 2 * count, axis=1) / (total_rows * narrow)
    place = lax.broadcasted_iota(jnp.int32, (1, LANES), 1)
    entries = jnp.where(
        place < count, float(total_rows * sq_cols * narrow), float(total_rows * na_cols * narrow)
    )
    spread = jnp.sqrt(mean * total / entries)
    scale = jnp.sqrt(mean) / jnp.maximum(1.0, spread / clip_limit)
    lane = lax.broadcasted_iota(jnp.int32, (2 * count, LANES), 1)
    sub = lax.broadcasted_iota(jnp.int32, (2 * count, LANES), 0)
    picked = jnp.sum(jnp.where(lane == sub, scale, 0.0), axis=1, keepdims=True)
    scale_out[...] = jnp.broadcast_to(picked, (2 * count, LANES))

    @pl.loop(1, devices)
    def _(d):
        fin_copy(me, d, lax.rem(me + d, devices)).wait_send()


def update_kernel(
    sq_g, na_g, sq_rf, sq_cf, na_rf, na_cf, scale,
    sq_out, na_out, sq_rf_out, sq_cf_out, na_rf_out, na_cf_out,
    sq_slots, na_slots, sq_sems, na_sems, small_sems,
):
    count, rows, sq_cols = sq_g.shape
    slots = sq_slots.shape[0]
    per = rows // LANES
    half = LANES // 2
    small = [
        pltpu.make_async_copy(src, dst, small_sems.at[i])
        for i, (src, dst) in enumerate(
            ((sq_rf, sq_rf_out), (sq_cf, sq_cf_out), (na_rf, na_rf_out), (na_cf, na_cf_out))
        )
    ]
    for copy in small:
        copy.start()
    kinds = (
        (sq_g, sq_rf, sq_cf, sq_out, sq_slots, sq_sems, 0),
        (na_g, na_rf, na_cf, na_out, na_slots, na_sems, count),
    )

    def out_copy(kind, t, h):
        _, _, _, out, held, sems, _ = kind
        slot = lax.rem(t, slots)
        row = pl.multiple_of(lax.rem(t, per) * LANES + h * half, half)
        return pltpu.make_async_copy(
            held.at[slot, pl.ds(h * half, half), :],
            out.at[lax.div(t, per), pl.ds(row, half), :],
            sems.at[slot, h],
        )

    def wait(t):
        for kind in kinds:
            for h in range(2):
                out_copy(kind, t, h).wait()

    @pl.loop(0, count * per)
    def _(t):
        m, q, slot = lax.div(t, per), lax.rem(t, per), lax.rem(t, slots)
        at = pl.multiple_of(q * LANES, LANES)

        @pl.when(t >= slots)
        def _():
            wait(t - slots)

        for kind in kinds:
            g, rf, cf, _, held, _, first = kind
            rowmul = lax.rsqrt(picked_row(rf[:, pl.ds(at, LANES)], m)) * scale[pl.ds(first + m, 1), :]
            rowmul = jnp.broadcast_to(rowmul, (LANES, LANES)).T
            cols = g.shape[2]
            block = min(cols, 512)
            for h in range(2):
                rows_at = pl.ds(pl.multiple_of(at + h * half, half), half)
                mul = rowmul[h * half : (h + 1) * half]
                for start in range(0, cols, block):
                    colmul = lax.rsqrt(cf[pl.ds(m, 1), pl.ds(start, block)])
                    values = g[m, rows_at, pl.ds(start, block)].astype(jnp.float32)
                    held[slot, pl.ds(h * half, half), pl.ds(start, block)] = (
                        values * tiled(mul, block // LANES) * colmul
                    )
                out_copy(kind, t, h).start()

    for t in range(max(count * per - slots, 0), count * per):
        wait(t)
    for copy in small:
        copy.wait()


def kernel_per_device(wide, narrow, square_grads, narrow_grads, *states):
    count, rows, sq_cols = square_grads.shape
    na_cols = narrow_grads.shape[2]
    f32 = jnp.float32
    vmem = pl.BlockSpec(memory_space=pltpu.VMEM)
    hbm = pl.BlockSpec(memory_space=pltpu.HBM)
    shape = jax.ShapeDtypeStruct
    table_rows = count * (sq_cols + na_cols) // LANES // wide
    chunks = count * (sq_cols // column_block(sq_cols) + na_cols // column_block(na_cols))
    dma = pltpu.SemaphoreType.DMA
    slots = 3
    factors = (
        shape((count, rows), f32),
        shape((count, sq_cols), f32),
        shape((count, rows), f32),
        shape((count, na_cols), f32),
    )
    *stats, square_held, narrow_held = pl.pallas_call(
        functools.partial(stats_kernel, wide, narrow),
        out_shape=factors
        + (
            shape((2 * count, LANES), f32),
            shape(square_grads.shape, square_grads.dtype),
            shape(narrow_grads.shape, narrow_grads.dtype),
        ),
        in_specs=[hbm] * 6,
        out_specs=[vmem] * 7,
        scratch_shapes=[
            pltpu.VMEM((count, rows), f32),
            pltpu.VMEM((count, sq_cols), f32),
            pltpu.VMEM((count, rows), f32),
            pltpu.VMEM((count, na_cols), f32),
            pltpu.VMEM((rows, LANES), f32),
            pltpu.VMEM((rows, LANES), f32),
            pltpu.VMEM((2 * count, rows // LANES, LANES), f32),
            pltpu.VMEM((2 * count, rows // LANES, LANES), f32),
            pltpu.VMEM((wide, table_rows, LANES), f32),
            pltpu.VMEM((wide, table_rows, LANES), f32),
            pltpu.VMEM((wide, table_rows, LANES), f32),
            pltpu.VMEM((count, 8, sq_cols), f32),
            pltpu.VMEM((count, 8, na_cols), f32),
            pltpu.VMEM((4 * count, LANES), f32),
            pltpu.VMEM((wide * narrow, 1, LANES), f32),
            dma((chunks,)),
            dma((4,)),
            dma((2 * count,)),
            dma((2 * count,)),
            dma((wide,)),
            dma((wide,)),
            dma((wide,)),
            dma((wide,)),
            dma((wide * narrow,)),
            dma((wide * narrow,)),
        ],
        compiler_params=pltpu.CompilerParams(
            collective_id=0, has_side_effects=True, vmem_limit_bytes=12 * 2**20
        ),
        name="stats",
    )(*(pltpu.with_memory_space_constraint(x, pltpu.HBM) for x in (square_grads, narrow_grads, *states)))

    return pl.pallas_call(
        update_kernel,
        out_shape=(
            shape(square_grads.shape, f32),
            shape(narrow_grads.shape, f32),
        )
        + factors,
        in_specs=[vmem] * 7,
        out_specs=[hbm] * 6,
        scratch_shapes=[
            pltpu.VMEM((slots, LANES, sq_cols), f32),
            pltpu.VMEM((slots, LANES, na_cols), f32),
            dma((slots, 2)),
            dma((slots, 2)),
            dma((4,)),
        ],
        compiler_params=pltpu.CompilerParams(vmem_limit_bytes=12 * 2**20),
        name="update",
    )(square_held, narrow_held, *stats)


def solution(mesh):
    wide, narrow = mesh.shape["wide"], mesh.shape["narrow"]

    def per_device(square_grads, narrow_grads, *states):
        count, rows, sq_cols = square_grads.shape
        na_cols = narrow_grads.shape[2]
        whole_tiles = (
            narrow == 2
            and wide > 1
            and rows % LANES == 0
            and sq_cols % (LANES * wide) == 0
            and na_cols % LANES == 0
            and sq_cols != na_cols
            and (count * na_cols) % (LANES * wide) == 0
            and 4 * count <= LANES
        )
        if whole_tiles:
            return kernel_per_device(wide, narrow, square_grads, narrow_grads, *states)
        return plain_per_device(square_grads, narrow_grads, *states)

    placed = (
        P(None, "wide", "narrow"),
        P(None, "wide", "narrow"),
        P(None, "wide"),
        P(None, "narrow"),
        P(None, "wide"),
        P(None, "narrow"),
    )
    return jax.shard_map(
        per_device,
        mesh=mesh,
        in_specs=placed,
        out_specs=placed,
        check_vma=False,
    )
```
